32 devices in a mesh: row: 2 (over x), col: 16 (over z, y, core).
Axes of the slice: x: 2, y: 2, z: 4, core: 2. Of those that a mesh axis runs over, the one named last changes fastest.
Arguments:
- adjacency: int32 [2048, 64], P('row', 'col'), may hold values from -2147483648 to 2147483647, as said below
- tile_mask: int32 [16, 16], P('row', 'col'), may hold values from 0 to 1, as said below
- thresholds: int32 [3], replicated, may hold values from 30 to 61
Outputs:
- truss_support: float32 [2048, 2048], P('row', 'col')
- edge_counts: int32 [3], replicated
The draws below stay inside these ranges and needn't reach their ends.
Inputs may be any that keep to these rules, and one draw needn't show every extreme that they name: The graph of adjacency is symmetric with an empty diagonal: bit b of word w of row i equals the bit for row 32 w + b and column i. `tile_mask`: Symmetric.
All inputs are finite; a program needn't handle non-finite values.
Results may differ from the reference program's by a relative error of at most 0.0003.
Values may be sent and summed in bfloat16 or wider, within the bound.
A program may use at most 64 MiB of HBM per device.

```python
import jax
import jax.numpy as jnp

TILE = 128
ITERS = 3
VERT = 2048


def draw_tile_mask(key, part):
    tiles = VERT // TILE
    base_group = jax.random.randint(jax.random.fold_in(key, 11), (tiles,), 0, 4)
    chooser = jax.random.randint(jax.random.fold_in(key, 12), (tiles,), 0, 3)
    community = jnp.where(chooser == 0, base_group, 0)
    extra_links = jax.random.randint(jax.random.fold_in(key, 13), (tiles, tiles), 0, 10)
    extra_links = jnp.minimum(extra_links, extra_links.T)
    same_group = community[:, None] == community[None, :]
    return jnp.where(same_group | (extra_links < 2), 1, 0).astype(jnp.int32)


def draw_adjacency(key, part):
    tiles = VERT // TILE
    density = jax.random.randint(jax.random.fold_in(key, 21), (tiles, tiles), 30, 400)
    density = (density + density.T) // 2
    level = jnp.repeat(jnp.repeat(density, TILE, axis=0), TILE, axis=1)
    roll = jax.random.randint(jax.random.fold_in(key, 22), (VERT, VERT), 0, 1000)
    vertex = jnp.arange(VERT, dtype=jnp.int32)
    upper = (roll < level) & (vertex[:, None] < vertex[None, :])
    full_graph = (upper | upper.T).astype(jnp.int32)
    shifts = jnp.arange(32, dtype=jnp.int32)
    shifted = jnp.left_shift(full_graph.reshape(VERT, VERT // 32, 32), shifts)
    return jnp.sum(shifted, axis=-1, dtype=jnp.int32).astype(jnp.int32)


def setup_inputs(seed: int = 0) -> dict:
    key_of = jax.random.split(jax.random.key(seed), 4)
    adjacency = draw_adjacency(jax.random.fold_in(key_of[3], 71), 0)
    tile_mask = draw_tile_mask(jax.random.fold_in(key_of[3], 71), 0)
    thresholds = jax.random.randint(key_of[2], (ITERS,), VERT * 15 // 1000, VERT * 30 // 1000 + 1).astype(jnp.int32)
    return dict(adjacency=adjacency, tile_mask=tile_mask, thresholds=thresholds)


def unpack_bits(packed_rows):
    shifts = jnp.arange(32, dtype=jnp.int32)
    flat_bits = jnp.bitwise_and(jnp.right_shift(packed_rows[:, :, None], shifts), 1)
    return flat_bits.reshape(packed_rows.shape[0], packed_rows.shape[1] * 32).astype(jnp.int32)


def reference(adjacency, tile_mask, thresholds):
    flat_bits = unpack_bits(adjacency)
    tile_cover = jnp.repeat(jnp.repeat(tile_mask, TILE, axis=0), TILE, axis=1).astype(jnp.int32)
    surviving = flat_bits * tile_cover
    survived_list = []
    support = jnp.zeros(surviving.shape, jnp.float32)
    for iteration in range(ITERS):
        operand = surviving.astype(jnp.bfloat16)
        wedge_counts = jnp.dot(operand, operand, preferred_element_type=jnp.float32)
        support = wedge_counts * surviving.astype(jnp.float32)
        retained = (support >= thresholds[iteration].astype(jnp.float32)).astype(jnp.int32)
        surviving = surviving * retained
        survived_list.append(jnp.sum(surviving).astype(jnp.int32))
    truss_support = support * surviving.astype(jnp.float32) / thresholds[ITERS - 1].astype(jnp.float32)
    return truss_support, jnp.stack(survived_list).astype(jnp.int32)
```

```python
import functools

import jax
import jax.numpy as jnp
from jax import lax
from jax.experimental import pallas as pl
from jax.experimental.pallas import tpu as pltpu
from jax.sharding import PartitionSpec as P

TILE = 128
ITERS = 3
BITS = 32
MESH = pl.DeviceIdType.MESH


def wrap(i, n):
    return jnp.where(i >= n, i - n, i)


def spread(load_row, words, width):
    bit = lax.broadcasted_iota(jnp.int32, (BITS, width), 0)
    parts = []
    for w in range(words):
        row = jnp.broadcast_to(load_row(w), (BITS, width))
        parts.append(jnp.bitwise_and(jnp.right_shift(row, bit), 1).astype(jnp.float32))
    return parts


def planes(words):
    return [jnp.bitwise_and(jnp.right_shift(words, b), 1).astype(jnp.float32) for b in range(BITS)]


def kernel(
    n_row, n_col, adj_ref, mask_ref, thr_ref, out_ref, count_ref,
    first, cols0, own, gath, cols, lhs, rhs, acc, tally, tallies, turned, landed,
    send_g, recv_g, send_h, recv_h, send_s, recv_s, send_x, recv_x,
    send_c, recv_c, send_o, recv_o, out_sem,
):
    words, rows = adj_ref.shape
    wide = 2 * words * BITS
    half = rows // 2
    pairs = n_col // 2
    n_dev = n_row * n_col
    my_row, my_col = lax.axis_index("row"), lax.axis_index("col")
    my_pair, my_core = my_col // 2, lax.rem(my_col, 2)
    other = 1 - my_core
    tiles_here = rows // TILE
    per_half = half // wide

    def shifted(pair, d, sign):
        slow = lax.rem(pair // 2 + sign * (d // 2) + pairs // 2, pairs // 2)
        return slow * 2 + lax.rem(pair + d, 2)

    def peer(dr, dc):
        return (wrap(my_row + dr, n_row), wrap(my_col + dc, n_col))

    def each_peer(body):
        if n_dev <= 64:
            for d in range(1, n_dev):
                body(d, peer(d // n_col, d % n_col))
        else:
            def step(d, c):
                body(d, peer(d // n_col, lax.rem(d, n_col)))
                return c

            lax.fori_loop(1, n_dev, step, 0)

    barrier = pltpu.get_barrier_semaphore()
    each_peer(
        lambda d, dev: pl.semaphore_signal(barrier, inc=1, device_id=dev, device_id_type=MESH)
    )

    cols0[my_row, my_core] = jnp.concatenate(
        [adj_ref[:, i * TILE : (i + 1) * TILE] * mask_ref[0, i] for i in range(tiles_here)], axis=1
    )
    pl.semaphore_wait(barrier, n_dev - 1)

    def remote(src, dst, send, recv, dev):
        return pltpu.make_async_remote_copy(
            src_ref=src, dst_ref=dst, send_sem=send, recv_sem=recv, device_id=dev, device_id_type=MESH
        )

    def block(t):
        return cols0.at[my_row, my_core] if t == 0 else own.at[t - 1]

    def gather(t, d, h):
        dev = (my_row, shifted(my_pair, d, 1) * 2 + (h if t == 0 else my_core))
        if t == 0:
            return remote(
                cols0.at[my_row, my_core, :, h * half : (h + 1) * half], first.at[my_pair, my_core],
                send_h.at[d, h], recv_h.at[d, my_core], dev,
            )
        return remote(own.at[t - 1], gath.at[t - 1, my_pair], send_g.at[t - 1, d], recv_g.at[t - 1, d], dev)

    def arrived(t, d):
        if t > 0:
            gather(t, d, 0).wait_recv()
        else:
            for c in range(2):
                src = shifted(my_pair, d, -1)
                remote(
                    first.at[src, c], first.at[src, c], send_h.at[d, c], recv_h.at[d, c], (my_row, my_col)
                ).wait_recv()

    def landing(t):
        return cols0.at[my_row, my_core] if t == 0 else cols.at[t - 1, my_row, my_core]

    def sibling(t):
        return remote(block(t), landing(t), send_s.at[t], recv_s.at[t], (my_row, my_pair * 2 + other))

    def across(t, d, c):
        return remote(
            block(t), landing(t), send_x.at[t, d, c], recv_x.at[t, d, my_core],
            (wrap(my_row + d, n_row), my_pair * 2 + c),
        )

    def across_arrived(t, d, c):
        return remote(
            block(t), landing(t), send_x.at[t, d, c], recv_x.at[t, d, c], (my_row, my_col)
        )

    far = lambda d: min(d // 2, pairs // 2 - d // 2) + d % 2
    order = sorted(range(1, pairs), key=lambda d: (far(d), d % 2))

    def multiply(t, group):
        k = 0
        left, total = [], 0
        for d in group:
            src = shifted(my_pair, d, -1)
            if d == 0:
                load = lambda s: own_words(t)[s : s + 1, :]
                if t > 0:
                    load = lambda s: own[t - 1, s : s + 1, :]
            elif t == 0:
                load = lambda s: first[src, s // words, s % words : s % words + 1, :]
            else:
                load = lambda s: gath[t - 1, src, s : s + 1, :]
            for s, part in enumerate(spread(load, 2 * words, half)):
                rhs[d, s * BITS : (s + 1) * BITS, :] = part.astype(jnp.bfloat16)
            left.append((src, d))
        for src, d in left:
            total = total + jnp.dot(lhs[src], rhs[d], preferred_element_type=jnp.float32)
        return total

    def own_words(t):
        if t > 0:
            return own[t - 1]
        rows_of = pl.ds(pl.multiple_of(my_core * half, half), half)
        return jnp.concatenate([cols0[my_row, c, :, rows_of] for c in range(2)], axis=0)

    def build(t, r):
        for h in range(2):
            if t == 0:
                part = jnp.concatenate(
                    [cols0[r, c, :, h * half : (h + 1) * half] for c in range(2)], axis=0
                )
            else:
                part = cols[t - 1, r, h]
            if t < ITERS - 1:
                full = jnp.concatenate(planes(part), axis=0)
            else:
                full = jnp.concatenate(
                    spread(lambda s: cols[t - 1, r, h, s : s + 1, :], 2 * words, half), axis=0
                )
            full = full.astype(jnp.bfloat16)
            for q in range(per_half):
                lhs[(r * 2 + h) * per_half + q] = full[:, q * wide : (q + 1) * wide]

    def lanes(v):
        total = v[:, :TILE]
        for i in range(1, v.shape[1] // TILE):
            total = total + v[:, i * TILE : (i + 1) * TILE]
        return jnp.sum(total, axis=0, keepdims=True)

    for t in range(ITERS):
        threshold = thr_ref[t].astype(jnp.float32)
        for d in range(1, n_row):
            for c in range(2):
                across(t, d, c).start()
        sibling(t).start()
        for d in reversed(order):
            for h in range(2 if t == 0 else 1):
                gather(t, d, h).start()

        sibling(t).wait_recv()
        for d in range(1, n_row):
            for c in range(2):
                across_arrived(t, d, c).wait_recv()
        for r in range(n_row):
            build(t, r)

        groups = [[0]]
        for i in range(0, len(order), 2):
            groups.append(order[i : i + 2])
        for i, group in enumerate(groups):
            for d in group:
                if d:
                    arrived(t, d)
            if i == 0:
                acc[...] = multiply(t, group)
            elif i < len(groups) - 1:
                acc[...] += multiply(t, group)
            else:
                wedges = acc[...] + multiply(t, group)

        held = own_words(t)
        if t < ITERS - 1:
            size = 2 * words
            stay = jnp.zeros_like(held)
            for b in range(BITS):
                bit = jnp.int32(-(2**31) if b == 31 else 2**b)
                stay = stay | jnp.where(wedges[b * size : (b + 1) * size, :] >= threshold, bit, 0)
            held = held & stay
            own[t] = held
            cols[t, my_row, my_core] = held
            tally[t : t + 1, :] = lanes(lax.population_count(held))
        else:
            live = jnp.concatenate(spread(lambda s: held[s : s + 1, :], 2 * words, half), axis=0)
            kept = (live > 0.0) & (wedges >= threshold)
            tally[t : t + 1, :] = lanes(jnp.where(kept, 1.0, 0.0)).astype(jnp.int32)

    def count(d, dev):
        return remote(tally, tallies.at[my_row * n_col + my_col], send_c.at[d], recv_c.at[d], dev)

    each_peer(lambda d, dev: count(d, dev).start())
    tallies[my_row * n_col + my_col] = tally[...]

    ratio = jnp.where(kept, wedges, 0.0) / threshold
    for c in range(2):
        for i in range(half // TILE):
            turned[c, i * TILE : (i + 1) * TILE, :] = ratio[
                c * (wide // 2) : (c + 1) * (wide // 2), i * TILE : (i + 1) * TILE
            ].T
    swap = remote(turned.at[other], landed, send_o, recv_o, (my_row, my_pair * 2 + other))
    swap.start()
    mine = pltpu.make_async_copy(
        turned.at[my_core], out_ref.at[pl.ds(pl.multiple_of(my_core * half, half), half)], out_sem.at[0]
    )
    mine.start()
    swap.wait_recv()
    theirs = pltpu.make_async_copy(
        landed, out_ref.at[pl.ds(pl.multiple_of(other * half, half), half)], out_sem.at[1]
    )
    theirs.start()

    for t in range(ITERS):
        for d in range(1, n_row):
            for c in range(2):
                across(t, d, c).wait_send()
        sibling(t).wait_send()
        for d in order:
            for h in range(2 if t == 0 else 1):
                gather(t, d, h).wait_send()
    swap.wait_send()
    each_peer(lambda d, dev: count(d, dev).wait())
    total = jnp.sum(jnp.sum(tallies[...], axis=0), axis=1, keepdims=True)
    for t in range(ITERS):
        count_ref[t] = total[t, 0]
    mine.wait()
    theirs.wait()


def local(n_row, n_col, adjacency, tile_mask, thresholds):
    packed = adjacency.T
    words, rows = packed.shape
    cols = words * BITS
    half = rows // 2
    n_dev = n_row * n_col
    pairs = n_col // 2
    dma = pltpu.SemaphoreType.DMA
    return pl.pallas_call(
        functools.partial(kernel, n_row, n_col),
        out_shape=(
            jax.ShapeDtypeStruct((rows, cols), jnp.float32),
            jax.ShapeDtypeStruct((ITERS,), jnp.int32),
        ),
        in_specs=[
            pl.BlockSpec(memory_space=pltpu.VMEM),
            pl.BlockSpec(memory_space=pltpu.SMEM),
            pl.BlockSpec(memory_space=pltpu.SMEM),
        ],
        out_specs=(
            pl.BlockSpec(memory_space=pl.ANY),
            pl.BlockSpec(memory_space=pltpu.SMEM),
        ),
        scratch_shapes=[
            pltpu.VMEM((pairs, 2, words, half), jnp.int32),
            pltpu.VMEM((n_row, 2, words, rows), jnp.int32),
            pltpu.VMEM((ITERS - 1, 2 * words, half), jnp.int32),
            pltpu.VMEM((ITERS - 1, pairs, 2 * words, half), jnp.int32),
            pltpu.VMEM((ITERS - 1, n_row, 2, 2 * words, half), jnp.int32),
            pltpu.VMEM((pairs, 2 * cols, 2 * cols), jnp.bfloat16),
            pltpu.VMEM((pairs, 2 * cols, half), jnp.bfloat16),
            pltpu.VMEM((2 * cols, half), jnp.float32),
            pltpu.VMEM((ITERS, TILE), jnp.int32),
            pltpu.VMEM((n_dev, ITERS, TILE), jnp.int32),
            pltpu.VMEM((2, half, cols), jnp.float32),
            pltpu.VMEM((half, cols), jnp.float32),
            dma((ITERS - 1, pairs)), dma((ITERS - 1, pairs)),
            dma((pairs, 2)), dma((pairs, 2)),
            dma((ITERS,)), dma((ITERS,)),
            dma((ITERS, n_row, 2)), dma((ITERS, n_row, 2)),
            dma((n_dev,)), dma((n_dev,)),
            dma, dma, dma((2,)),
        ],
        compiler_params=pltpu.CompilerParams(collective_id=0, has_side_effects=True),
    )(packed, tile_mask.T, thresholds)


def solution(mesh):
    in_specs = (P("row", "col"), P("row", "col"), P())
    out_specs = (P("row", "col"), P())
    body = functools.partial(local, mesh.shape["row"], mesh.shape["col"])
    return jax.shard_map(body, mesh=mesh, in_specs=in_specs, out_specs=out_specs, check_vma=False)
```

```python
import functools

import jax
import jax.numpy as jnp
from jax import lax
from jax.experimental import pallas as pl
from jax.experimental.pallas import tpu as pltpu
from jax.sharding import PartitionSpec as P

TILE = 128
ITERS = 3
BITS = 32
MESH = pl.DeviceIdType.MESH


def wrap(i, n):
    return jnp.where(i >= n, i - n, i)


def spread(load_row, words, width):
    bit = lax.broadcasted_iota(jnp.int32, (BITS, width), 0)
    parts = []
    for w in range(words):
        row = jnp.broadcast_to(load_row(w), (BITS, width))
        parts.append(jnp.bitwise_and(jnp.right_shift(row, bit), 1).astype(jnp.float32))
    return parts


def planes(words):
    return [jnp.bitwise_and(jnp.right_shift(words, b), 1).astype(jnp.float32) for b in range(BITS)]


def kernel(
    n_row, n_col, adj_hbm, mask_hbm, thr_hbm, out_ref, count_ref, adj_ref, mask_ref, thr_ref,
    first, cols0, own, gath, cols, lhs, rhs, acc, tally, tallies, turned, landed,
    send_g, recv_g, send_h, recv_h, send_s, recv_s, send_x, recv_x,
    send_c, recv_c, send_o, recv_o, load_sem,
):
    words, rows = adj_ref.shape
    wide = 2 * words * BITS
    half = rows // 2
    pairs = n_col // 2
    n_dev = n_row * n_col
    my_row, my_col = lax.axis_index("row"), lax.axis_index("col")
    my_pair, my_core = my_col // 2, lax.rem(my_col, 2)
    other = 1 - my_core
    tiles_here = rows // TILE
    per_half = half // wide

    depth = (pairs - 1).bit_length()
    swaps = pairs == 2**depth

    def shifted(pair, d, sign):
        if swaps:
            return sum(lax.rem(pair // 2**i + d // 2**i % 2, 2) * 2**i for i in range(depth))
        return lax.rem(pair + sign * d + pairs, pairs)

    def peer(dr, dc):
        return (wrap(my_row + dr, n_row), wrap(my_col + dc, n_col))

    def each_peer(body):
        if n_dev <= 64:
            for d in range(1, n_dev):
                body(d, peer(d // n_col, d % n_col))
        else:
            def step(d, c):
                body(d, peer(d // n_col, lax.rem(d, n_col)))
                return c

            lax.fori_loop(1, n_dev, step, 0)

    loads = [
        pltpu.make_async_copy(src, dst, load_sem.at[i])
        for i, (src, dst) in enumerate(((adj_hbm, adj_ref), (mask_hbm, mask_ref), (thr_hbm, thr_ref)))
    ]
    for load in loads:
        load.start()

    barrier = pltpu.get_barrier_semaphore()
    near = [peer(0, d) for d in range(1, n_col)]
    near += [(wrap(my_row + d, n_row), my_pair * 2 + c) for d in range(1, n_row) for c in range(2)]
    for dev in near:
        pl.semaphore_signal(barrier, inc=1, device_id=dev, device_id_type=MESH)
    for load in loads:
        load.wait()

    cols0[my_row, my_core] = jnp.concatenate(
        [adj_ref[:, i * TILE : (i + 1) * TILE] * mask_ref[0, i] for i in range(tiles_here)], axis=1
    )
    pl.semaphore_wait(barrier, len(near))

    def remote(src, dst, send, recv, dev):
        return pltpu.make_async_remote_copy(
            src_ref=src, dst_ref=dst, send_sem=send, recv_sem=recv, device_id=dev, device_id_type=MESH
        )

    def block(t):
        return cols0.at[my_row, my_core] if t == 0 else own.at[t - 1]

    def gather(t, d, h):
        dev = (my_row, shifted(my_pair, d, 1) * 2 + (h if t == 0 else my_core))
        if t == 0:
            return remote(
                cols0.at[my_row, my_core, :, h * half : (h + 1) * half], first.at[my_pair, my_core],
                send_h.at[d, h], recv_h.at[d, my_core], dev,
            )
        return remote(own.at[t - 1], gath.at[t - 1, my_pair], send_g.at[t - 1, d], recv_g.at[t - 1, d], dev)

    def arrived(t, d):
        if t > 0:
            gather(t, d, 0).wait_recv()
        else:
            for c in range(2):
                src = shifted(my_pair, d, -1)
                remote(
                    first.at[src, c], first.at[src, c], send_h.at[d, c], recv_h.at[d, c], (my_row, my_col)
                ).wait_recv()

    def landing(t):
        return cols0.at[my_row, my_core] if t == 0 else cols.at[t - 1, my_row, my_core]

    def sibling(t):
        return remote(block(t), landing(t), send_s.at[t], recv_s.at[t], (my_row, my_pair * 2 + other))

    def across(t, d, c):
        return remote(
            block(t), landing(t), send_x.at[t, d, c], recv_x.at[t, d, my_core],
            (wrap(my_row + d, n_row), my_pair * 2 + c),
        )

    def across_arrived(t, d, c):
        return remote(
            block(t), landing(t), send_x.at[t, d, c], recv_x.at[t, d, c], (my_row, my_col)
        )

    order = sorted(range(1, pairs), key=lambda d: d // 2 + d % 2)

    def multiply(t, group):
        k = 0
        left, total = [], 0
        for d in group:
            src = shifted(my_pair, d, -1)
            if d == 0:
                load = lambda s: own_words(t)[s : s + 1, :]
                if t > 0:
                    load = lambda s: own[t - 1, s : s + 1, :]
            elif t == 0:
                load = lambda s: first[src, s // words, s % words : s % words + 1, :]
            else:
                load = lambda s: gath[t - 1, src, s : s + 1, :]
            for s, part in enumerate(spread(load, 2 * words, half)):
                rhs[d, s * BITS : (s + 1) * BITS, :] = part.astype(jnp.bfloat16)
            left.append((src, d))
        for src, d in left:
            total = total + jnp.dot(lhs[src], rhs[d], preferred_element_type=jnp.float32)
        return total

    def own_words(t):
        if t > 0:
            return own[t - 1]
        rows_of = pl.ds(pl.multiple_of(my_core * half, half), half)
        return jnp.concatenate([cols0[my_row, c, :, rows_of] for c in range(2)], axis=0)

    def build(t, r):
        for h in range(2):
            if t == 0:
                part = jnp.concatenate(
                    [cols0[r, c, :, h * half : (h + 1) * half] for c in range(2)], axis=0
                )
            else:
                part = cols[t - 1, r, h]
            if t < ITERS - 1:
                full = jnp.concatenate(planes(part), axis=0)
            else:
                full = jnp.concatenate(
                    spread(lambda s: cols[t - 1, r, h, s : s + 1, :], 2 * words, half), axis=0
                )
            full = full.astype(jnp.bfloat16)
            for q in range(per_half):
                lhs[(r * 2 + h) * per_half + q] = full[:, q * wide : (q + 1) * wide]

    def lanes(v):
        total = v[:, :TILE]
        for i in range(1, v.shape[1] // TILE):
            total = total + v[:, i * TILE : (i + 1) * TILE]
        return jnp.sum(total, axis=0, keepdims=True)

    for t in range(ITERS):
        threshold = thr_ref[t].astype(jnp.float32)
        for d in range(1, n_row):
            for c in range(2):
                across(t, d, c).start()
        sibling(t).start()
        for d in reversed(order):
            for h in range(2 if t == 0 else 1):
                gather(t, d, h).start()

        sibling(t).wait_recv()
        for d in range(1, n_row):
            for c in range(2):
                across_arrived(t, d, c).wait_recv()
        for r in range(n_row):
            build(t, r)

        groups = [[0]]
        for i in range(0, len(order), 2):
            groups.append(order[i : i + 2])
        for i, group in enumerate(groups):
            for d in group:
                if d:
                    arrived(t, d)
            if i == 0:
                acc[...] = multiply(t, group)
            elif i < len(groups) - 1:
                acc[...] += multiply(t, group)
            else:
                wedges = acc[...] + multiply(t, group)

        held = own_words(t)
        if t < ITERS - 1:
            size = 2 * words
            stay = jnp.zeros_like(held)
            for b in range(BITS):
                bit = jnp.int32(-(2**31) if b == 31 else 2**b)
                stay = stay | jnp.where(wedges[b * size : (b + 1) * size, :] >= threshold, bit, 0)
            held = held & stay
            own[t] = held
            cols[t, my_row, my_core] = held
            tally[t : t + 1, :] = lanes(lax.population_count(held))
        else:
            live = jnp.concatenate(spread(lambda s: held[s : s + 1, :], 2 * words, half), axis=0)
            kept = (live > 0.0) & (wedges >= threshold)
            tally[t : t + 1, :] = lanes(jnp.where(kept, 1.0, 0.0)).astype(jnp.int32)

    def count(d, dev):
        return remote(tally, tallies.at[my_row * n_col + my_col], send_c.at[d], recv_c.at[d], dev)

    each_peer(lambda d, dev: count(d, dev).start())
    tallies[my_row * n_col + my_col] = tally[...]

    ratio = jnp.where(kept, wedges, 0.0) / threshold
    for c in range(2):
        for i in range(half // TILE):
            turned[c, i * TILE : (i + 1) * TILE, :] = ratio[
                c * (wide // 2) : (c + 1) * (wide // 2), i * TILE : (i + 1) * TILE
            ].T
    swap = remote(turned.at[other], landed, send_o, recv_o, (my_row, my_pair * 2 + other))
    swap.start()
    out_ref[pl.ds(pl.multiple_of(my_core * half, half), half), :] = turned[my_core]
    swap.wait_recv()
    out_ref[pl.ds(pl.multiple_of(other * half, half), half), :] = landed[...]
    for t in range(ITERS):
        for d in range(1, n_row):
            for c in range(2):
                across(t, d, c).wait_send()
        sibling(t).wait_send()
        for d in order:
            for h in range(2 if t == 0 else 1):
                gather(t, d, h).wait_send()
    swap.wait_send()
    each_peer(lambda d, dev: count(d, dev).wait())
    total = jnp.sum(jnp.sum(tallies[...], axis=0), axis=1, keepdims=True)
    for t in range(ITERS):
        count_ref[t] = total[t, 0]


def local(n_row, n_col, adjacency, tile_mask, thresholds):
    packed = adjacency.T
    words, rows = packed.shape
    cols = words * BITS
    half = rows // 2
    n_dev = n_row * n_col
    pairs = n_col // 2
    dma = pltpu.SemaphoreType.DMA
    return pl.pallas_call(
        functools.partial(kernel, n_row, n_col),
        out_shape=(
            pltpu.VMEM((rows, cols), jnp.float32),
            pltpu.SMEM((ITERS,), jnp.int32),
        ),
        in_specs=[
            pl.BlockSpec(memory_space=pl.ANY),
            pl.BlockSpec(memory_space=pl.ANY),
            pl.BlockSpec(memory_space=pl.ANY),
        ],
        out_specs=(
            pl.BlockSpec(memory_space=pltpu.VMEM),
            pl.BlockSpec(memory_space=pltpu.SMEM),
        ),
        scratch_shapes=[
            pltpu.VMEM((words, rows), jnp.int32),
            pltpu.SMEM((1, rows // TILE), jnp.int32),
            pltpu.SMEM((ITERS,), jnp.int32),
            pltpu.VMEM((pairs, 2, words, half), jnp.int32),
            pltpu.VMEM((n_row, 2, words, rows), jnp.int32),
            pltpu.VMEM((ITERS - 1, 2 * words, half), jnp.int32),
            pltpu.VMEM((ITERS - 1, pairs, 2 * words, half), jnp.int32),
            pltpu.VMEM((ITERS - 1, n_row, 2, 2 * words, half), jnp.int32),
            pltpu.VMEM((pairs, 2 * cols, 2 * cols), jnp.bfloat16),
            pltpu.VMEM((pairs, 2 * cols, half), jnp.bfloat16),
            pltpu.VMEM((2 * cols, half), jnp.float32),
            pltpu.VMEM((ITERS, TILE), jnp.int32),
            pltpu.VMEM((n_dev, ITERS, TILE), jnp.int32),
            pltpu.VMEM((2, half, cols), jnp.float32),
            pltpu.VMEM((half, cols), jnp.float32),
            dma((ITERS - 1, pairs)), dma((ITERS - 1, pairs)),
            dma((pairs, 2)), dma((pairs, 2)),
            dma((ITERS,)), dma((ITERS,)),
            dma((ITERS, n_row, 2)), dma((ITERS, n_row, 2)),
            dma((n_dev,)), dma((n_dev,)),
            dma, dma, dma((3,)),
        ],
        compiler_params=pltpu.CompilerParams(collective_id=0, has_side_effects=True),
    )(packed, tile_mask.T, thresholds)


def solution(mesh):
    in_specs = (P("row", "col"), P("row", "col"), P())
    out_specs = (P("row", "col"), P())
    body = functools.partial(local, mesh.shape["row"], mesh.shape["col"])
    return jax.shard_map(body, mesh=mesh, in_specs=in_specs, out_specs=out_specs, check_vma=False)
```
